512 devices in a mesh: seq: 64 (over z, x, core), tp: 8 (over y).
Axes of the slice: x: 4, y: 8, z: 8, core: 2. Of those that a mesh axis runs over, the one named last changes fastest.
Arguments:
- hidden_in: bfloat16 [8192, 4096], P('seq', 'tp'), may hold values from -64 to 64
- span_order: int32 [64], replicated, may hold values from 0 to 63, each once
- norm_gain: bfloat16 [4096], P('tp'), may hold values from 0.099609375 to 1.8984375
- w_query: bfloat16 [4096, 4096], P('seq', 'tp'), may hold values from -0.09375 to 0.09375
- bias_query: bfloat16 [4096], P('tp'), may hold values from -14 to 14
- key_value_weight: bfloat16 [4096, 2, 1024], P('seq', None, 'tp'), may hold values from -0.09375 to 0.09375
- bias_kv: bfloat16 [2, 1024], P(None, 'tp'), may hold values from -14 to 14
- w_out: bfloat16 [4096, 4096], P('tp', 'seq'), may hold values from -0.09375 to 0.09375
- post_gain: bfloat16 [4096], P('tp'), may hold values from 0.099609375 to 1.8984375
Outputs:
- attn_out: bfloat16 [8192, 4096], P('seq', 'tp')
- normed: bfloat16 [8192, 4096], P('seq', 'tp')
The draws below stay inside these ranges and needn't reach their ends.
Inputs may be any that keep to these rules, and one draw needn't show every extreme that they name: Each span number appears once; row r of hidden_in belongs to span span_order[r // 128].
All inputs are finite; a program needn't handle non-finite values.
Results may differ from the reference program's by a relative error of at most 0.014.
Values may be sent and summed in bfloat16 or wider, within the bound.
No kernel may reach another device: no remote copies, remote signals or barrier semaphores. Data moves between devices by JAX's collectives and lax.ppermute only.
A program may use at most 64 MiB of HBM per device.

```python
import math
import jax
import jax.numpy as jnp
from jax import lax

MODEL_WIDTH = 4096
QUERY_HEADS = 32
KEY_VALUE_HEADS = 8
HEAD_SIZE = 128
GROUP = 4
TOK_DEV = 128
SEQ = 8192
N_SEQ = 64
N_TP = 8


def draw_hidden_in(key, part):
    base_key, column_key, row_key = jax.random.split(key, 3)
    column_ids = jnp.arange(MODEL_WIDTH, dtype=jnp.float32) / MODEL_WIDTH
    base = jnp.clip(jax.random.normal(base_key, (SEQ, MODEL_WIDTH), jnp.float32), -4.0, 4.0)
    ramp = jnp.exp(0.5 * math.log(3.0) * column_ids)
    ramp = ramp / jnp.mean(ramp)
    columns = jnp.exp(jax.random.uniform(column_key, (MODEL_WIDTH,), jnp.float32, -1.1513, 1.1513))
    rows = jnp.exp(jax.random.uniform(row_key, (SEQ, 1), jnp.float32, -1.1513, 1.1513))
    field = jnp.clip(base * rows * (columns * ramp)[None, :], -64.0, 64.0)
    return field.astype(jnp.bfloat16)


def draw_bias_query(key, part):
    random_jitter = jax.random.normal(jax.random.fold_in(key, 11), (QUERY_HEADS * HEAD_SIZE,), jnp.float32)
    return jnp.clip(0.5 * random_jitter, -2.0, 2.0).astype(jnp.bfloat16)


def draw_bias_kv(key, part):
    random_jitter = jax.random.normal(jax.random.fold_in(key, 13), (2, KEY_VALUE_HEADS * HEAD_SIZE), jnp.float32)
    return jnp.clip(0.5 * random_jitter, -2.0, 2.0).astype(jnp.bfloat16)


def steps_of(stream_key, extent, pieces, low, top_value):
    factor_of = 1.0
    for position, shards_of in pieces:
        heights = jax.random.uniform(jax.random.fold_in(jax.random.fold_in(stream_key, 6), position), (shards_of,), jnp.float32, low / len(pieces), top_value / len(pieces))
        factor_of = factor_of * jnp.repeat(jnp.exp(heights), extent[position] // shards_of).reshape((-1,) + (1,) * (len(extent) - 1 - position))
    return factor_of


def noise(rng, dims, deviation, most, cuts=(), held_as=jnp.bfloat16):
    factor_of = steps_of(rng, dims, cuts, -0.22, 0.18) if cuts else 1.0
    result = jax.random.normal(rng, dims, jnp.float32) * deviation * factor_of
    return jnp.minimum(jnp.maximum(result, -most), most).astype(held_as)


def setup_inputs(seed: int = 0) -> dict:
    arg_keys = jax.random.split(jax.random.key(seed), 10)
    hidden_in = draw_hidden_in(jax.random.fold_in(arg_keys[9], 71), 0)
    span_order = jax.random.permutation(arg_keys[1], N_SEQ).astype(jnp.int32)
    norm_gain = jnp.clip(1.0 + 0.18 * jax.random.normal(arg_keys[2], (MODEL_WIDTH,), jnp.float32), 0.099609375, 1.8984375).astype(jnp.bfloat16)
    w_query = noise(arg_keys[3], (MODEL_WIDTH, QUERY_HEADS * HEAD_SIZE), MODEL_WIDTH ** -0.5, 0.09375, ((0, 64), (1, 8)))
    bias_query = draw_bias_query(jax.random.fold_in(arg_keys[9], 71), 0)
    key_value_weight = noise(arg_keys[5], (MODEL_WIDTH, 2, KEY_VALUE_HEADS * HEAD_SIZE), MODEL_WIDTH ** -0.5, 0.09375, ((0, 64), (2, 8)))
    bias_kv = draw_bias_kv(jax.random.fold_in(arg_keys[9], 71), 0)
    w_out = noise(arg_keys[7], (QUERY_HEADS * HEAD_SIZE, MODEL_WIDTH), (QUERY_HEADS * HEAD_SIZE) ** -0.5, 0.09375, ((0, 8), (1, 64)))
    post_gain = jnp.clip(1.0 + 0.18 * jax.random.normal(arg_keys[8], (MODEL_WIDTH,), jnp.float32), 0.099609375, 1.8984375).astype(jnp.bfloat16)
    return dict(hidden_in=hidden_in, span_order=span_order, norm_gain=norm_gain, w_query=w_query, bias_query=bias_query, key_value_weight=key_value_weight, bias_kv=bias_kv, w_out=w_out, post_gain=post_gain)


eps = 1e-06
rope_base = 1000000.0

def apply_rotary(field, token_positions):
    half = field.shape[-1] // 2
    inverse = jnp.exp(-math.log(rope_base) * jnp.arange(half, dtype=jnp.float32) / half)
    angles = token_positions.astype(jnp.float32)[:, None] * inverse[None, :]
    cosine = jnp.cos(angles)[:, None, :]
    sine = jnp.sin(angles)[:, None, :]
    first = field[..., :half]
    second = field[..., half:]
    return jnp.concatenate([first * cosine - second * sine, second * cosine + first * sine], axis=-1)

def reference(hidden_in, span_order, norm_gain, w_query, bias_query, key_value_weight, bias_kv, w_out, post_gain):
    sequence_length = hidden_in.shape[0]
    row_ids = jnp.arange(sequence_length, dtype=jnp.int32)
    token_positions = (span_order[row_ids // TOK_DEV] * TOK_DEV + row_ids % TOK_DEV).astype(jnp.int32)
    local = hidden_in.astype(jnp.float32)
    meansq = lax.optimization_barrier(jnp.mean(local * local, axis=1, keepdims=True))
    normed_in = (local * lax.rsqrt(meansq + eps) * norm_gain.astype(jnp.float32)[None, :]).astype(jnp.bfloat16)
    query_proj = jnp.dot(normed_in, w_query, preferred_element_type=jnp.float32) + bias_query.astype(jnp.float32)[None, :]
    queries = apply_rotary(query_proj.reshape(sequence_length, QUERY_HEADS, HEAD_SIZE), token_positions).astype(jnp.bfloat16)
    key_projected = jnp.dot(normed_in, key_value_weight[:, 0, :], preferred_element_type=jnp.float32) + bias_kv[0].astype(jnp.float32)[None, :]
    value_projected = jnp.dot(normed_in, key_value_weight[:, 1, :], preferred_element_type=jnp.float32) + bias_kv[1].astype(jnp.float32)[None, :]
    rotated_keys = apply_rotary(key_projected.reshape(sequence_length, KEY_VALUE_HEADS, HEAD_SIZE), token_positions).astype(jnp.bfloat16)
    value_rows = value_projected.astype(jnp.bfloat16).reshape(sequence_length, KEY_VALUE_HEADS, HEAD_SIZE)
    query_major = queries.transpose(1, 0, 2)
    key_major = jnp.repeat(rotated_keys.transpose(1, 0, 2), GROUP, axis=0)
    value_major = jnp.repeat(value_rows.transpose(1, 0, 2), GROUP, axis=0)
    allowed = token_positions[None, :] <= token_positions[:, None]
    scale = 1.0 / math.sqrt(HEAD_SIZE)

    def one_head(triple):
        query_one, key_one, value_one = triple
        scores = jnp.dot(query_one, key_one.T, preferred_element_type=jnp.float32) * scale
        scores = jnp.where(allowed, scores, -jnp.inf)
        peak = lax.optimization_barrier(jnp.max(scores, axis=1, keepdims=True))
        weights = jnp.where(allowed, jnp.exp(scores - peak), 0.0)
        totals = lax.optimization_barrier(jnp.sum(weights, axis=1, keepdims=True))
        summed = jnp.dot(weights.astype(jnp.bfloat16), value_one, preferred_element_type=jnp.float32)
        return (summed / totals).astype(jnp.bfloat16)
    attended = lax.map(one_head, (query_major, key_major, value_major))
    attended = attended.transpose(1, 0, 2).reshape(sequence_length, QUERY_HEADS * HEAD_SIZE)
    part_rows = QUERY_HEADS * HEAD_SIZE // N_TP
    mixed = jnp.zeros((sequence_length, MODEL_WIDTH), jnp.float32)
    for group in range(N_TP):
        lower = group * part_rows
        piece = jnp.dot(attended[:, lower:lower + part_rows], w_out[lower:lower + part_rows, :], preferred_element_type=jnp.float32)
        mixed = mixed + lax.optimization_barrier(piece.astype(jnp.bfloat16)).astype(jnp.float32)
    attn_out = mixed.astype(jnp.bfloat16)
    stream = local + mixed
    post_sq = lax.optimization_barrier(jnp.mean(stream * stream, axis=1, keepdims=True))
    normed = (stream * lax.rsqrt(post_sq + eps) * post_gain.astype(jnp.float32)[None, :]).astype(jnp.bfloat16)
    return (attn_out, normed)
```

```python
import functools
import math

import jax
import jax.numpy as jnp
from jax import lax
from jax.experimental import pallas as pl
from jax.experimental.pallas import tpu as pltpu
from jax.sharding import Mesh
from jax.sharding import PartitionSpec as P

MODEL_WIDTH = 4096
HEAD = 128
TOK = 128
GROUP = 4
NZ, NX, NC, NY = 8, 4, 2, 8
SEQ = ("z", "x", "c")
EPS = 1e-06
ROPE_BASE = 1000000.0
NEG = -(2.0**100)
F32 = jnp.float32
BF16 = jnp.bfloat16


def whole():
    return pl.BlockSpec(memory_space=pltpu.VMEM)


def scalars():
    return pl.BlockSpec(memory_space=pltpu.SMEM)


def call(kernel, out_shape, in_specs, name, scratch=()):
    outs = jax.tree.map(lambda _: whole(), out_shape)
    return pl.pallas_call(
        kernel,
        out_shape=out_shape,
        in_specs=in_specs,
        out_specs=outs,
        scratch_shapes=list(scratch),
        name=name,
    )


def split_sum(value):
    high = value.astype(BF16).astype(F32)
    rest = value - high
    middle = rest.astype(BF16).astype(F32)
    return high, middle, (rest - middle)


def rows_of(terms, count):
    width = terms[0].shape[1]
    ids = lax.broadcasted_iota(jnp.int32, (count, width), 0)
    out = jnp.zeros((count, width), F32)
    for k, term in enumerate(terms):
        out = jnp.where(ids == k, jnp.broadcast_to(term, (count, width)), out)
    return out.astype(BF16)


def row_sums(square):
    part = square[:, 0:128] + square[:, 128:256] + square[:, 256:384] + square[:, 384:512]
    return jnp.sum(part.T, axis=0, keepdims=True)


def prepare(h_ref, g_ref, wq_ref, wkv_ref, p_ref, w_ref):
    h = h_ref[...].astype(F32)
    tail = rows_of(split_sum(row_sums(h * h)), 8)
    scaled = (h * g_ref[...].astype(F32)).T
    for x in range(NX):
        block = scaled[x * 128 : (x + 1) * 128, :].astype(BF16)
        for y in range(NY):
            p_ref[x * NY + y, 0:128, :] = block
            p_ref[x * NY + y, 128:136, :] = tail
    w_ref[:, 0:512] = wq_ref[...]
    w_ref[:, 512:640] = wkv_ref[:, 0, :]
    w_ref[:, 640:768] = wkv_ref[:, 1, :]


def project(at_ref, x_ref, *refs):
    w_refs, (out_ref, xs_ref) = refs[:8], refs[8:]
    scales = []
    for x in range(NX):
        total = jnp.zeros((1, 128), F32)
        for y in range(NY):
            tail = x_ref[x * NY + y, 128:136, :].astype(F32)
            total += tail[0:1] + tail[1:2] + tail[2:3]
        scales.append(lax.rsqrt(total / MODEL_WIDTH + EPS))
    scale = jnp.concatenate(scales, axis=1)
    for k in range(8):
        y = at_ref[k]
        for x in range(NX):
            xs_ref[k * 128 : (k + 1) * 128, x * 128 : (x + 1) * 128] = x_ref[x * NY + y, 0:128, :]
    weights = jnp.concatenate([w[...] for w in w_refs], axis=0)
    out = lax.dot_general(
        weights, xs_ref[...], (((0,), (0,)), ((), ())), preferred_element_type=F32
    )
    out = (out * scale).astype(BF16)
    for x in range(NX):
        out_ref[x] = out[:, x * 128 : (x + 1) * 128]


def rotate(r_ref, b_ref, cos_ref, sin_ref, q_ref, kv_ref):
    def total(low, high):
        out = b_ref[low:high, :]
        for x in range(NX):
            out = out + r_ref[x, low:high, :].astype(F32)
        return out

    cos, sin = cos_ref[...], sin_ref[...]

    def turned(head):
        first = total(head * 128, head * 128 + 64)
        second = total(head * 128 + 64, head * 128 + 128)
        return jnp.concatenate(
            [first * cos - second * sin, second * cos + first * sin], axis=0
        )

    for head in range(GROUP):
        q_ref[:, head * 128 : (head + 1) * 128] = turned(head).astype(BF16)
    key = turned(GROUP).T.astype(BF16)
    value = total(640, 768).astype(BF16)
    for z in range(NZ):
        kv_ref[z, 0:128, :] = key
        kv_ref[z, 128:256, :] = value


def attend(order_ref, at_ref, q0, q1, q2, q3, kv0, kv1, o_ref, s_ref, p_ref):
    z, x, c = at_ref[0], at_ref[1], at_ref[2]
    key_spans = [order_ref[k * 8 + x * 2 + c] for k in range(NZ)]
    key_spans += [order_ref[k * 8 + x * 2 + 1 - c] for k in range(NZ)]
    values = jnp.concatenate(
        [kv[k, 128:256, :] for kv in (kv0, kv1) for k in range(NZ)], axis=1
    )
    gap = lax.broadcasted_iota(jnp.int32, (128, 512), 0) - (
        lax.broadcasted_iota(jnp.int32, (128, 512), 1) & 127
    )
    factor = math.log2(math.e) / math.sqrt(HEAD)
    for step, q in ((0, q0), (3, q1), (1, q2), (2, q3)):
        owner = (x + step) & 3
        span = order_ref[z * 8 + owner * 2 + c]
        queries = q[...]
        top = jnp.full((8, 512), NEG, F32)
        for k in range(16):
            kv = kv0 if k < 8 else kv1
            s = jnp.dot(kv[k % 8, 0:128, :], queries, preferred_element_type=F32)
            s = jnp.where(gap <= (span - key_spans[k]) * TOK, s * factor, NEG)
            s_ref[k * 128 : (k + 1) * 128, :] = s
            top = jnp.maximum(top, jnp.max(s.reshape(16, 8, 512), axis=0))
        high, low, _ = split_sum(jnp.max(top, axis=0, keepdims=True))
        low = low.astype(BF16).astype(F32)
        peak = high + low
        sums = jnp.zeros((8, 512), F32)
        for k in range(16):
            p = jnp.exp2(s_ref[k * 128 : (k + 1) * 128, :] - peak)
            sums = sums + jnp.sum(p.reshape(16, 8, 512), axis=0)
            p_ref[k * 128 : (k + 1) * 128, :] = p.astype(BF16)
        out = jnp.dot(values, p_ref[...], preferred_element_type=F32)
        total = split_sum(jnp.sum(sums, axis=0, keepdims=True))
        o_ref[pl.ds(owner, 1), 0:128, :] = out.astype(BF16)[None]
        o_ref[pl.ds(owner, 1), 128:144, :] = rows_of((high, low) + total, 16)[None]


def project_out(o_ref, w_ref, out_ref, a_ref):
    @pl.when(pl.program_id(0) == 0)
    def _():
        tails = [o_ref[x, 128:144, :].astype(F32) for x in range(NX)]
        peaks = [t[0:1] + t[1:2] for t in tails]
        top = functools.reduce(jnp.maximum, peaks)
        shares = [jnp.exp2(peak - top) for peak in peaks]
        total = sum(s * (t[2:3] + t[3:4] + t[4:5]) for s, t in zip(shares, tails))
        out = sum(s * o_ref[x, 0:128, :].astype(F32) for x, s in enumerate(shares)) / total
        out = out.astype(BF16)
        for head in range(GROUP):
            a_ref[head * 128 : (head + 1) * 128, :] = out[:, head * 128 : (head + 1) * 128]

    out_ref[0] = jnp.dot(w_ref[...], a_ref[...], preferred_element_type=F32).astype(BF16)


def mix(part_ref, h_ref, attn_ref, stream_ref, sq_ref):
    mixed = part_ref[0].astype(F32)
    for y in range(1, NY):
        mixed = mixed + part_ref[y].astype(F32)
    mixed = mixed.T
    attn_ref[...] = mixed.astype(BF16)
    stream = h_ref[...].astype(F32) + mixed
    stream_ref[...] = stream
    sums = row_sums(stream * stream)
    for y in range(NY):
        sq_ref[y] = sums


def finish(stream_ref, sq_ref, g_ref, out_ref):
    total = sq_ref[0]
    for y in range(1, NY):
        total = total + sq_ref[y]
    scale = lax.rsqrt(total / MODEL_WIDTH + EPS)
    scale = jnp.broadcast_to(scale, (128, 128)).T
    gain = g_ref[...].astype(F32)
    for k in range(4):
        cols = slice(k * 128, (k + 1) * 128)
        out_ref[:, cols] = (stream_ref[:, cols] * scale * gain[:, cols]).astype(BF16)


def shifted(array, axis, step):
    size = lax.axis_size(axis)
    return lax.ppermute(array, axis, [(i, (i + step) % size) for i in range(size)])


def per_device(
    hidden_in,
    span_order,
    norm_gain,
    w_query,
    bias_query,
    key_value_weight,
    bias_kv,
    w_out,
    post_gain,
):
    shape = jax.ShapeDtypeStruct
    z, x, c = (lax.axis_index(a) for a in SEQ)
    at = jnp.stack([z, x, c]).astype(jnp.int32)
    own = z * 8 + x * 2 + c

    w_out_all = lax.all_gather(w_out.T, SEQ, axis=0, tiled=True)

    pieces, w_own = call(
        prepare,
        (shape((NX * NY, 136, 128), BF16), shape((64, 768), BF16)),
        [whole()] * 4,
        "prepare",
    )(hidden_in, norm_gain.reshape(1, 512), w_query, key_value_weight)
    arrived = lax.all_to_all(pieces, ("x", "tp"), 0, 0, tiled=True)

    w_other = shifted(w_own, "c", 1)
    pair = jnp.where(
        c == 0, jnp.concatenate([w_own, w_other], 0), jnp.concatenate([w_other, w_own], 0)
    )
    ring = []
    for k in range(NZ):
        ring += [(k * 2, ((k + 1) % NZ) * 2), (k * 2 + 1, ((k + NZ - 1) % NZ) * 2 + 1)]
    held = [pair]
    for _ in range(4):
        held.append(lax.ppermute(held[-1], ("z", "c"), ring))
    crossed = [shifted(held[k], "c", 1) for k in (1, 2, 3)]
    sign = 2 * c - 1
    sources = jnp.stack(
        [z]
        + [(z + sign * k) % NZ for k in (1, 2, 3, 4)]
        + [(z - sign * k) % NZ for k in (1, 2, 3)]
    ).astype(jnp.int32)
    projected = call(
        project,
        shape((NX, 768, 128), BF16),
        [scalars()] + [whole()] * 9,
        "project",
        [pltpu.VMEM((1024, 512), BF16)],
    )(sources, arrived, *held, *crossed)
    shares = lax.all_to_all(projected, "x", 0, 0, tiled=True)

    ids = jnp.arange(span_order.shape[0], dtype=jnp.int32)
    own_span = jnp.sum(jnp.where(ids == own, span_order, 0))
    positions = own_span * TOK + jnp.arange(TOK, dtype=jnp.int32)
    half = HEAD // 2
    inverse = jnp.exp(-math.log(ROPE_BASE) * jnp.arange(half, dtype=F32) / half)
    angles = inverse[:, None] * positions.astype(F32)[None, :]
    bias = jnp.concatenate([bias_query, bias_kv.reshape(256)]).astype(F32)
    bias = jnp.broadcast_to(bias[:, None], (768, 128))
    queries, kv = call(
        rotate,
        (shape((128, 512), BF16), shape((NZ, 256, 128), BF16)),
        [whole()] * 4,
        "rotate",
    )(shares, bias, jnp.cos(angles), jnp.sin(angles))

    kv_here = lax.all_to_all(kv, "z", 0, 0, tiled=True)
    others = [shifted(queries, "x", step) for step in (1, -1, 2)]
    kv_there = shifted(kv_here, "c", 1)
    partial = call(
        attend,
        shape((NX, 144, 512), BF16),
        [scalars()] * 2 + [whole()] * 6,
        "attend",
        [pltpu.VMEM((2048, 512), F32), pltpu.VMEM((2048, 512), BF16)],
    )(span_order, at, queries, *others, kv_here, kv_there)
    partial = lax.all_to_all(partial, "x", 0, 0, tiled=True)

    out = pl.pallas_call(
        project_out,
        grid=(NY,),
        out_shape=shape((NY, 512, 128), BF16),
        in_specs=[
            pl.BlockSpec((NX, 144, 512), lambda i: (0, 0, 0)),
            pl.BlockSpec((512, 512), lambda i: (i, 0)),
        ],
        out_specs=pl.BlockSpec((1, 512, 128), lambda i: (i, 0, 0)),
        scratch_shapes=[pltpu.VMEM((512, 128), BF16)],
        name="project_out",
    )(partial, w_out_all)
    out = lax.all_to_all(out, "tp", 0, 0, tiled=True)

    attn_out, stream, squares = call(
        mix,
        (shape((128, 512), BF16), shape((128, 512), F32), shape((NY, 1, 128), F32)),
        [whole()] * 2,
        "mix",
    )(out, hidden_in)
    squares = lax.all_to_all(squares, "tp", 0, 0, tiled=True)
    normed = call(finish, shape((128, 512), BF16), [whole()] * 3, "finish")(
        stream, squares, post_gain.reshape(1, 512)
    )
    return attn_out, normed


def solution(mesh):
    torus = Mesh(mesh.devices.reshape(NZ, NX, NC, NY), ("z", "x", "c", "tp"))
    in_specs = (
        P(SEQ, "tp"),
        P(),
        P("tp"),
        P(SEQ, "tp"),
        P("tp"),
        P(SEQ, None, "tp"),
        P(None, "tp"),
        P("tp", SEQ),
        P("tp"),
    )
    out_specs = (P(SEQ, "tp"), P(SEQ, "tp"))
    return jax.shard_map(
        per_device, mesh=torus, in_specs=in_specs, out_specs=out_specs, check_vma=False
    )
```

```python
import functools
import math

import jax
import jax.numpy as jnp
from jax import lax
from jax.experimental import pallas as pl
from jax.experimental.pallas import tpu as pltpu
from jax.sharding import Mesh
from jax.sharding import PartitionSpec as P


MODEL_WIDTH = 4096
HEAD = 128
TOK = 128
GROUP = 4
NZ, NX, NC, NY = 8, 4, 2, 8
SEQ = ("z", "x", "c")
EPS = 1e-06
ROPE_BASE = 1000000.0
NEG = -(2.0**100)
F32 = jnp.float32
BF16 = jnp.bfloat16


def call(kernel, outs, *args, scratch=(), kept=(), free=(), far=(), limit=24):
    specs, given = [], []
    for k, a in enumerate(args):
        if a.dtype == jnp.int32:
            specs.append(pl.BlockSpec(memory_space=pltpu.SMEM))
        else:
            specs.append(pl.BlockSpec(memory_space=pltpu.VMEM))
            if k not in free:
                space = pltpu.HBM if k in far else pltpu.VMEM
                a = pltpu.with_memory_space_constraint(a, space)
        given.append(a)
    shapes = [
        jax.ShapeDtypeStruct(s, d) if k in kept else pltpu.VMEM(s, d)
        for k, (s, d) in enumerate(outs)
    ]
    spec = [pl.BlockSpec(memory_space=pltpu.VMEM)] * len(outs)
    return pl.pallas_call(
        kernel,
        out_shape=shapes,
        in_specs=specs,
        out_specs=spec,
        scratch_shapes=list(scratch),
        compiler_params=pltpu.CompilerParams(vmem_limit_bytes=limit << 20),
    )(*given)


def split_sum(value):
    high = value.astype(BF16).astype(F32)
    rest = value - high
    middle = rest.astype(BF16).astype(F32)
    return high, middle, (rest - middle)


def rows_of(terms, count):
    width = terms[0].shape[1]
    ids = lax.broadcasted_iota(jnp.int32, (count, width), 0)
    out = jnp.zeros((count, width), F32)
    for k, term in enumerate(terms):
        out = jnp.where(ids == k, jnp.broadcast_to(term, (count, width)), out)
    return out.astype(BF16)


def row_sums(square):
    part = square[:, 0:128] + square[:, 128:256] + square[:, 256:384] + square[:, 384:512]
    return jnp.sum(part.T, axis=0, keepdims=True)


def prepare(h_ref, g_ref, p_ref):
    h = h_ref[...].astype(F32)
    tail = rows_of(split_sum(row_sums(h * h)), 8)
    scaled = (h * g_ref[...].astype(F32).reshape(1, 512)).T
    for x in range(NX):
        block = scaled[x * 128 : (x + 1) * 128, :].astype(BF16)
        for y in range(NY):
            p_ref[x * NY + y, 0:128, :] = block
            p_ref[x * NY + y, 128:136, :] = tail


def stack_weights(wq_ref, wkv_ref, wo_ref, w_ref):
    w_ref[:, 0:512] = wq_ref[...]
    w_ref[:, 512:640] = wkv_ref[:, 0, :]
    w_ref[:, 640:768] = wkv_ref[:, 1, :]
    w_ref[:, 768:1280] = wo_ref[...]


def sources(z, c):
    sign = 2 * c - 1
    near = [z] + [z + sign * k for k in (1, 2, 3, 4)] + [z - sign * k for k in (1, 2, 3)]
    return [(n + NZ) & (NZ - 1) for n in near]


def project(x_ref, *refs):
    w_refs, (out_ref, xs_ref) = refs[:8], refs[8:]
    c = lax.axis_index("c")
    at = sources(lax.axis_index("z"), c)
    scales = []
    for x in range(NX):
        total = jnp.zeros((1, 128), F32)
        for y in range(NY):
            tail = x_ref[x * NY + y, 128:136, :].astype(F32)
            total += tail[0:1] + tail[1:2] + tail[2:3]
        scales.append(lax.rsqrt(total / MODEL_WIDTH + EPS))
    scale = jnp.concatenate(scales, axis=1)
    for k in range(8):
        for x in range(NX):
            block = x_ref[pl.ds(x * NY + at[k], 1), 0:128, :].reshape(128, 128)
            xs_ref[k * 128 : (k + 1) * 128, x * 128 : (x + 1) * 128] = block
    weights = jnp.concatenate([w[...] for w in w_refs], axis=0)
    out = lax.dot_general(
        weights, xs_ref[...], (((0,), (0,)), ((), ())), preferred_element_type=F32
    )
    out = (out * scale).astype(BF16)
    for x in range(NX):
        out_ref[x] = out[:, x * 128 : (x + 1) * 128]


def rotate(r_ref, b_ref, cos_ref, sin_ref, q_ref, kv_ref):
    def total(low, high):
        out = b_ref[low:high, :]
        for x in range(NX):
            out = out + r_ref[x, low:high, :].astype(F32)
        return out

    cos, sin = cos_ref[...], sin_ref[...]

    def turned(head):
        first = total(head * 128, head * 128 + 64)
        second = total(head * 128 + 64, head * 128 + 128)
        return jnp.concatenate(
            [first * cos - second * sin, second * cos + first * sin], axis=0
        )

    for head in range(GROUP):
        q_ref[:, head * 128 : (head + 1) * 128] = turned(head).astype(BF16)
    key = turned(GROUP).T.astype(BF16)
    value = total(640, 768).astype(BF16)
    for z in range(NZ):
        kv_ref[z, 0:128, :] = key
        kv_ref[z, 128:256, :] = value


def attend(order_ref, q0, q1, q2, q3, kv0, kv1, o_ref, s_ref, p_ref):
    z, x, c = (lax.axis_index(a) for a in SEQ)
    key_spans = [order_ref[k * 8 + x * 2 + c] for k in range(NZ)]
    key_spans += [order_ref[k * 8 + x * 2 + 1 - c] for k in range(NZ)]
    values = jnp.concatenate(
        [kv[k, 128:256, :] for kv in (kv0, kv1) for k in range(NZ)], axis=1
    )
    gap = lax.broadcasted_iota(jnp.int32, (128, 512), 0) - (
        lax.broadcasted_iota(jnp.int32, (128, 512), 1) & 127
    )
    factor = math.log2(math.e) / math.sqrt(HEAD)
    for step, q in ((0, q0), (3, q1), (1, q2), (2, q3)):
        owner = (x + step) & 3
        span = order_ref[z * 8 + owner * 2 + c]
        queries = q[...]
        top = jnp.full((8, 512), NEG, F32)
        for k in range(16):
            kv = kv0 if k < 8 else kv1
            s = jnp.dot(kv[k % 8, 0:128, :], queries, preferred_element_type=F32)
            s = jnp.where(gap <= (span - key_spans[k]) * TOK, s * factor, NEG)
            s_ref[k * 128 : (k + 1) * 128, :] = s
            top = jnp.maximum(top, jnp.max(s.reshape(16, 8, 512), axis=0))
        high, low, _ = split_sum(jnp.max(top, axis=0, keepdims=True))
        low = low.astype(BF16).astype(F32)
        peak = high + low
        sums = jnp.zeros((8, 512), F32)
        for k in range(16):
            p = jnp.exp2(s_ref[k * 128 : (k + 1) * 128, :] - peak)
            sums = sums + jnp.sum(p.reshape(16, 8, 512), axis=0)
            p_ref[k * 128 : (k + 1) * 128, :] = p.astype(BF16)
        out = jnp.dot(values, p_ref[...], preferred_element_type=F32)
        total = split_sum(jnp.sum(sums, axis=0, keepdims=True))
        o_ref[pl.ds(owner, 1), 0:128, :] = out.astype(BF16)[None]
        o_ref[pl.ds(owner, 1), 128:144, :] = rows_of((high, low) + total, 16)[None]


def pick(*refs):
    out_ref = refs[5]
    c = lax.axis_index("c")

    @pl.when(c == 0)
    def _():
        for k in range(4):
            out_ref[k * 128 : (k + 1) * 128, :] = refs[k][...]

    @pl.when(c != 0)
    def _():
        for k in range(4):
            out_ref[k * 128 : (k + 1) * 128, :] = refs[k + 1][...]


def tables(bq_ref, bkv_ref, b_ref):
    for k in range(4):
        row = bq_ref[:, k * 128 : (k + 1) * 128].astype(F32)
        b_ref[k * 128 : (k + 1) * 128, :] = jnp.broadcast_to(row, (128, 128)).T
    for k in range(2):
        row = bkv_ref[k : k + 1, :].astype(F32)
        b_ref[512 + k * 128 : 640 + k * 128, :] = jnp.broadcast_to(row, (128, 128)).T


def project_out(o_ref, *refs):
    w_refs, (out_ref, a_ref) = refs[:8], refs[8:]
    z, x, c = (lax.axis_index(a) for a in SEQ)
    tails = [o_ref[k, 128:144, :].astype(F32) for k in range(NX)]
    peaks = [t[0:1] + t[1:2] for t in tails]
    top = functools.reduce(jnp.maximum, peaks)
    shares = [jnp.exp2(peak - top) for peak in peaks]
    total = sum(s * (t[2:3] + t[3:4] + t[4:5]) for s, t in zip(shares, tails))
    out = sum(s * o_ref[k, 0:128, :].astype(F32) for k, s in enumerate(shares)) / total
    out = out.astype(BF16)
    for head in range(GROUP):
        a_ref[head * 128 : (head + 1) * 128, :] = out[:, head * 128 : (head + 1) * 128]
    low = [(z - k + NZ) & (NZ - 1) for k in range(4)]
    high = [(z + 1 + k) & (NZ - 1) for k in range(4)]
    for k in range(8):
        owner = (x + (0, 3, 1, 2)[k % 4]) & 3
        part = jnp.dot(w_refs[k][...], a_ref[...], preferred_element_type=F32).astype(BF16)
        for n in range(4):
            mine, other = (low[n], high[n]) if k < 4 else (high[n], low[n])
            y = jnp.where(c == 0, mine, other)
            rows = pl.ds(pl.multiple_of(owner * 128, 128), 128)
            out_ref[pl.ds(y, 1), rows, :] = part[n * 128 : (n + 1) * 128, :][None]


def copied(in_ref, out_ref):
    out_ref[...] = in_ref[...].astype(F32)


def spread(in_ref, out_ref):
    out_ref[...] = jnp.broadcast_to(in_ref[...], (8, 512))


def mix(part_ref, h_ref, attn_ref, stream_ref, sq_ref):
    mixed = part_ref[0].astype(F32)
    for y in range(1, NY):
        mixed = mixed + part_ref[y].astype(F32)
    mixed = mixed.T
    attn_ref[...] = mixed.astype(BF16)
    stream = h_ref[...] + mixed
    stream_ref[...] = stream
    sums = row_sums(stream * stream)
    for y in range(NY):
        sq_ref[y] = sums


def finish(stream_ref, sq_ref, g_ref, out_ref):
    total = sq_ref[0]
    for y in range(1, NY):
        total = total + sq_ref[y]
    scale = lax.rsqrt(total / MODEL_WIDTH + EPS)
    scale = jnp.broadcast_to(scale, (128, 128)).T
    gain = g_ref[0:1, :]
    for k in range(4):
        cols = slice(k * 128, (k + 1) * 128)
        out_ref[:, cols] = (stream_ref[:, cols] * scale * gain[:, cols]).astype(BF16)


def shifted(array, axis, step):
    size = lax.axis_size(axis)
    return lax.ppermute(array, axis, [(i, (i + step) % size) for i in range(size)])


def exchanged(array, axis):
    return lax.all_to_all(array, axis, 0, 0, tiled=True)


def moved(array, axis, step=1):
    return shifted(array, axis, step)


def layer(
    hidden_in,
    span_order,
    norm_gain,
    w_query,
    bias_query,
    key_value_weight,
    bias_kv,
    w_out,
    post_gain,
):
    z, x, c = (lax.axis_index(a) for a in SEQ)
    own = z * 8 + x * 2 + c

    (w_own,) = call(
        stack_weights,
        [((64, 1280), BF16)],
        w_query,
        key_value_weight,
        w_out.T,
        far=(0, 1, 2),
    )
    w_other = moved(w_own, "c")
    (pieces,) = call(
        prepare, [((NX * NY, 136, 128), BF16)], hidden_in, norm_gain, far=(0, 1)
    )
    arrived = exchanged(pieces, ("x", "tp"))
    pair = jnp.where(
        c == 0, jnp.concatenate([w_own, w_other], 0), jnp.concatenate([w_other, w_own], 0)
    )
    ring = []
    for k in range(NZ):
        ring += [(k * 2, ((k + 1) % NZ) * 2), (k * 2 + 1, ((k + NZ - 1) % NZ) * 2 + 1)]
    held, wo_held = [pair[:, :768]], [pair[:, 768:]]
    for _ in range(4):
        held.append(lax.ppermute(held[-1], ("z", "c"), ring))
        wo_held.append(lax.ppermute(wo_held[-1], ("z", "c"), ring))
    crossed = [moved(held[k], "c") for k in (1, 2, 3)]
    (projected,) = call(
        project,
        [((NX, 768, 128), BF16)],
        arrived,
        *held,
        *crossed,
        scratch=[pltpu.VMEM((1024, 512), BF16)],
        free=range(1, 9),
    )
    (wo_here,) = call(pick, [((512, 512), BF16)], *wo_held)
    shares = exchanged(projected, "x")

    ids = jnp.arange(span_order.shape[0], dtype=jnp.int32)
    own_span = jnp.sum(jnp.where(ids == own, span_order, 0))
    positions = own_span * TOK + jnp.arange(TOK, dtype=jnp.int32)
    half = HEAD // 2
    inverse = jnp.exp(-math.log(ROPE_BASE) * jnp.arange(half, dtype=F32) / half)
    angles = inverse[:, None] * positions.astype(F32)[None, :]
    (residual,) = call(copied, [((128, 512), F32)], hidden_in, far=(0,))
    (bias,) = call(tables, [((768, 128), F32)], bias_query.reshape(1, 512), bias_kv)
    queries, kv = call(
        rotate,
        [((128, 512), BF16), ((NZ, 256, 128), BF16)],
        shares,
        bias,
        jnp.cos(angles),
        jnp.sin(angles),
    )

    wo_there = moved(wo_here, "c")
    kv_here = exchanged(kv, "z")
    others = [moved(queries, "x", step) for step in (1, -1, 2)]
    wo_x = [wo_here] + [moved(wo_here, "x", step) for step in (1, -1, 2)]
    (widened,) = call(copied, [((1, 512), F32)], post_gain.reshape(1, 512))
    kv_there = moved(kv_here, "c")
    (partial,) = call(
        attend,
        [((NX, 144, 512), BF16)],
        span_order,
        queries,
        *others,
        kv_here,
        kv_there,
        scratch=[pltpu.VMEM((2048, 512), F32), pltpu.VMEM((2048, 512), BF16)],
    )
    partial = exchanged(partial, "x")
    wo_c = [wo_there] + [moved(w, "c") for w in wo_x[1:]]
    (gains,) = call(spread, [((8, 512), F32)], widened)
    (out,) = call(
        project_out,
        [((NY, 512, 128), BF16)],
        partial,
        *wo_x,
        *wo_c,
        scratch=[pltpu.VMEM((512, 128), BF16)],
    )
    out = exchanged(out, "tp")

    attn_out, stream, squares = call(
        mix,
        [((128, 512), BF16), ((128, 512), F32), ((NY, 1, 128), F32)],
        out,
        residual,
        kept=(0,),
    )
    squares = exchanged(squares, "tp")
    (normed,) = call(finish, [((128, 512), BF16)], stream, squares, gains, kept=(0,))
    return attn_out, normed


def solution(mesh):
    torus = Mesh(mesh.devices.reshape(NZ, NX, NC, NY), ("z", "x", "c", "tp"))
    in_specs = (
        P(SEQ, "tp"),
        P(),
        P("tp"),
        P(SEQ, "tp"),
        P("tp"),
        P(SEQ, None, "tp"),
        P(None, "tp"),
        P("tp", SEQ),
        P("tp"),
    )
    out_specs = (P(SEQ, "tp"), P(SEQ, "tp"))
    return jax.shard_map(
        layer, mesh=torus, in_specs=in_specs, out_specs=out_specs, check_vma=False
    )
```

```python
import functools
import math

import jax
import jax.numpy as jnp
from jax import lax
from jax.experimental import pallas as pl
from jax.experimental.pallas import tpu as pltpu
from jax.sharding import Mesh
from jax.sharding import PartitionSpec as P


MODEL_WIDTH = 4096
HEAD = 128
TOK = 128
GROUP = 4
NZ, NX, NC, NY = 8, 4, 2, 8
SEQ = ("z", "x", "c")
TP = ("tq", "tr")
EPS = 1e-06
ROPE_BASE = 1000000.0
NEG = -(2.0**100)
F32 = jnp.float32
BF16 = jnp.bfloat16


def call(kernel, outs, *args, scratch=(), kept=(), free=(), far=(), limit=24):
    specs, given = [], []
    for k, a in enumerate(args):
        if a.dtype == jnp.int32:
            specs.append(pl.BlockSpec(memory_space=pltpu.SMEM))
        else:
            specs.append(pl.BlockSpec(memory_space=pltpu.VMEM))
            if k not in free:
                space = pltpu.HBM if k in far else pltpu.VMEM
                a = pltpu.with_memory_space_constraint(a, space)
        given.append(a)
    shapes = [
        jax.ShapeDtypeStruct(s, d) if k in kept else pltpu.VMEM(s, d)
        for k, (s, d) in enumerate(outs)
    ]
    spec = [pl.BlockSpec(memory_space=pltpu.VMEM)] * len(outs)
    return pl.pallas_call(
        kernel,
        out_shape=shapes,
        in_specs=specs,
        out_specs=spec,
        scratch_shapes=list(scratch),
        compiler_params=pltpu.CompilerParams(vmem_limit_bytes=limit << 20),
    )(*given)


def split_sum(value):
    high = value.astype(BF16).astype(F32)
    rest = value - high
    middle = rest.astype(BF16).astype(F32)
    return high, middle, (rest - middle)


def rows_of(terms, count):
    width = terms[0].shape[1]
    ids = lax.broadcasted_iota(jnp.int32, (count, width), 0)
    out = jnp.zeros((count, width), F32)
    for k, term in enumerate(terms):
        out = jnp.where(ids == k, jnp.broadcast_to(term, (count, width)), out)
    return out.astype(BF16)


def row_sums(square):
    part = square[:, 0:128] + square[:, 128:256] + square[:, 256:384] + square[:, 384:512]
    return jnp.sum(part.T, axis=0, keepdims=True)


def prepare(h_ref, g_ref, p_ref):
    h = h_ref[...].astype(F32)
    tail = rows_of(split_sum(row_sums(h * h)), 8)
    scaled = (h * g_ref[...].astype(F32).reshape(1, 512)).T
    for x in range(NX):
        block = scaled[x * 128 : (x + 1) * 128, :].astype(BF16)
        for y in range(NY):
            p_ref[x * NY + y, 0:128, :] = block
            p_ref[x * NY + y, 128:136, :] = tail


def stack_weights(wq_ref, wkv_ref, wo_ref, w_ref):
    w_ref[:, 0:512] = wq_ref[...]
    w_ref[:, 512:640] = wkv_ref[:, 0, :]
    w_ref[:, 640:768] = wkv_ref[:, 1, :]
    w_ref[:, 768:1280] = wo_ref[...]


def sources(z, c):
    sign = 2 * c - 1
    near = [z] + [z + sign * k for k in (1, 2, 3, 4)] + [z - sign * k for k in (1, 2, 3)]
    return [(n + NZ) & (NZ - 1) for n in near]


def project(x_ref, *refs):
    w_refs, (out_ref, xs_ref) = refs[:8], refs[8:]
    c = lax.axis_index("c")
    at = sources(lax.axis_index("z"), c)
    scales = []
    for x in range(NX):
        total = jnp.zeros((1, 128), F32)
        for y in range(NY):
            tail = x_ref[x * NY + y, 128:136, :].astype(F32)
            total += tail[0:1] + tail[1:2] + tail[2:3]
        scales.append(lax.rsqrt(total / MODEL_WIDTH + EPS))
    scale = jnp.concatenate(scales, axis=1)
    for k in range(8):
        for x in range(NX):
            block = x_ref[pl.ds(x * NY + at[k], 1), 0:128, :].reshape(128, 128)
            xs_ref[k * 128 : (k + 1) * 128, x * 128 : (x + 1) * 128] = block
    weights = jnp.concatenate([w[...] for w in w_refs], axis=0)
    out = lax.dot_general(
        weights, xs_ref[...], (((0,), (0,)), ((), ())), preferred_element_type=F32
    )
    out = (out * scale).astype(BF16)
    for x in range(NX):
        out_ref[x] = out[:, x * 128 : (x + 1) * 128]


def rotate(r_ref, b_ref, cos_ref, sin_ref, q_ref, kv_ref):
    def total(low, high):
        out = b_ref[low:high, :]
        for x in range(NX):
            out = out + r_ref[x, low:high, :].astype(F32)
        return out

    cos, sin = cos_ref[...], sin_ref[...]

    def turned(head):
        first = total(head * 128, head * 128 + 64)
        second = total(head * 128 + 64, head * 128 + 128)
        return jnp.concatenate(
            [first * cos - second * sin, second * cos + first * sin], axis=0
        )

    for head in range(GROUP):
        q_ref[:, head * 128 : (head + 1) * 128] = turned(head).astype(BF16)
    key = turned(GROUP).T.astype(BF16)
    value = total(640, 768).astype(BF16)
    for z in range(NZ):
        kv_ref[z, 0:128, :] = key
        kv_ref[z, 128:256, :] = value


def attend(order_ref, q0, q1, q2, q3, kv0, kv1, o_ref, s_ref, p_ref):
    z, x, c = (lax.axis_index(a) for a in SEQ)
    key_spans = [order_ref[k * 8 + x * 2 + c] for k in range(NZ)]
    key_spans += [order_ref[k * 8 + x * 2 + 1 - c] for k in range(NZ)]
    values = jnp.concatenate(
        [kv[k, 128:256, :] for kv in (kv0, kv1) for k in range(NZ)], axis=1
    )
    gap = lax.broadcasted_iota(jnp.int32, (128, 512), 0) - (
        lax.broadcasted_iota(jnp.int32, (128, 512), 1) & 127
    )
    factor = math.log2(math.e) / math.sqrt(HEAD)
    for step, q in ((0, q0), (3, q1), (1, q2), (2, q3)):
        owner = (x + step) & 3
        span = order_ref[z * 8 + owner * 2 + c]
        queries = q[...]
        top = jnp.full((8, 512), NEG, F32)
        for k in range(16):
            kv = kv0 if k < 8 else kv1
            s = jnp.dot(kv[k % 8, 0:128, :], queries, preferred_element_type=F32)
            s = jnp.where(gap <= (span - key_spans[k]) * TOK, s * factor, NEG)
            s_ref[k * 128 : (k + 1) * 128, :] = s
            top = jnp.maximum(top, jnp.max(s.reshape(16, 8, 512), axis=0))
        high, low, _ = split_sum(jnp.max(top, axis=0, keepdims=True))
        low = low.astype(BF16).astype(F32)
        peak = high + low
        sums = jnp.zeros((8, 512), F32)
        for k in range(16):
            p = jnp.exp2(s_ref[k * 128 : (k + 1) * 128, :] - peak)
            sums = sums + jnp.sum(p.reshape(16, 8, 512), axis=0)
            p_ref[k * 128 : (k + 1) * 128, :] = p.astype(BF16)
        out = jnp.dot(values, p_ref[...], preferred_element_type=F32)
        total = split_sum(jnp.sum(sums, axis=0, keepdims=True))
        o_ref[pl.ds(owner, 1), 0:128, :] = out.astype(BF16)[None]
        o_ref[pl.ds(owner, 1), 128:144, :] = rows_of((high, low) + total, 16)[None]


def same_parity():
    return (lax.axis_index("z") & 1) == lax.axis_index("tr")


def pick(h1, h2, h3, out_ref):
    late = jnp.logical_and(same_parity(), lax.axis_index("c") == 1)

    @pl.when(late)
    def _():
        out_ref[0:256, :] = h2[...]
        out_ref[256:512, :] = h3[...]

    @pl.when(jnp.logical_not(late))
    def _():
        out_ref[0:256, :] = h1[...]
        out_ref[256:512, :] = h2[...]


def tables(bq_ref, bkv_ref, b_ref):
    for k in range(4):
        row = bq_ref[:, k * 128 : (k + 1) * 128].astype(F32)
        b_ref[k * 128 : (k + 1) * 128, :] = jnp.broadcast_to(row, (128, 128)).T
    for k in range(2):
        row = bkv_ref[k : k + 1, :].astype(F32)
        b_ref[512 + k * 128 : 640 + k * 128, :] = jnp.broadcast_to(row, (128, 128)).T


def merge(o_ref, a_ref):
    tails = [o_ref[k, 128:144, :].astype(F32) for k in range(NX)]
    peaks = [t[0:1] + t[1:2] for t in tails]
    top = functools.reduce(jnp.maximum, peaks)
    shares = [jnp.exp2(peak - top) for peak in peaks]
    total = sum(s * (t[2:3] + t[3:4] + t[4:5]) for s, t in zip(shares, tails))
    out = sum(s * o_ref[k, 0:128, :].astype(F32) for k, s in enumerate(shares)) / total
    out = out.astype(BF16)
    for head in range(GROUP):
        a_ref[head * 128 : (head + 1) * 128, :] = out[:, head * 128 : (head + 1) * 128]


def project_out(a_own, a_other, *refs):
    w_refs, (out_ref, a_ref) = refs[:8], refs[8:]
    z, x, c = (lax.axis_index(a) for a in SEQ)
    side = lax.axis_index("tr")
    a_ref[pl.ds(side, 1)] = a_own[...][None]
    a_ref[pl.ds(1 - side, 1)] = a_other[...][None]
    attended = a_ref[...].reshape(1024, 128)
    same = jnp.where(same_parity(), 1, 0)
    low, high = z - 1 + same, z + 1 + same
    for core in range(2):
        rows = []
        for k in range(4):
            w = w_refs[core * 4 + k]
            for n in range(2):
                at = n * 256
                rows.append(jnp.concatenate([w[at : at + 128, :], w[at + 128 : at + 256, :]], axis=1))
        part = jnp.dot(
            jnp.concatenate(rows, axis=0), attended, preferred_element_type=F32
        ).astype(BF16)
        for k in range(4):
            owner = (x + (0, 3, 1, 2)[k]) & 3
            cols = pl.ds(pl.multiple_of(owner * 128, 128), 128)
            for n in range(2):
                block = jnp.where(c == core, low - 2 * n, high + 2 * n)
                y = ((block + NZ) & (NZ - 1)) >> 1
                at = (k * 2 + n) * 128
                out_ref[pl.ds(y, 1), cols, :] = part[at : at + 128, :][None]


def copied(in_ref, out_ref):
    out_ref[...] = in_ref[...].astype(F32)


def spread(in_ref, out_ref):
    out_ref[...] = jnp.broadcast_to(in_ref[...], (8, 512))


def mix(part_ref, h_ref, attn_ref, stream_ref, sq_ref):
    mixed = part_ref[0].astype(F32)
    for y in range(1, NY // 2):
        mixed = mixed + part_ref[y].astype(F32)
    mixed = mixed.T
    attn_ref[...] = mixed.astype(BF16)
    stream = h_ref[...] + mixed
    stream_ref[...] = stream
    sums = row_sums(stream * stream)
    for y in range(NY):
        sq_ref[y] = sums


def finish(stream_ref, sq_ref, g_ref, out_ref):
    total = sq_ref[0]
    for y in range(1, NY):
        total = total + sq_ref[y]
    scale = lax.rsqrt(total / MODEL_WIDTH + EPS)
    scale = jnp.broadcast_to(scale, (128, 128)).T
    gain = g_ref[0:1, :]
    for k in range(4):
        cols = slice(k * 128, (k + 1) * 128)
        out_ref[:, cols] = (stream_ref[:, cols] * scale * gain[:, cols]).astype(BF16)


def shifted(array, axis, step):
    size = lax.axis_size(axis)
    return lax.ppermute(array, axis, [(i, (i + step) % size) for i in range(size)])


def exchanged(array, axis):
    return lax.all_to_all(array, axis, 0, 0, tiled=True)


def moved(array, axis, step=1):
    return shifted(array, axis, step)


def layer(
    hidden_in,
    span_order,
    norm_gain,
    w_query,
    bias_query,
    key_value_weight,
    bias_kv,
    w_out,
    post_gain,
):
    z, x, c = (lax.axis_index(a) for a in SEQ)
    own = z * 8 + x * 2 + c

    (w_own,) = call(
        stack_weights,
        [((64, 1280), BF16)],
        w_query,
        key_value_weight,
        w_out.T,
        far=(0, 1, 2),
    )
    w_other = moved(w_own, "c")
    (pieces,) = call(
        prepare, [((NX * NY, 136, 128), BF16)], hidden_in, norm_gain, far=(0, 1)
    )
    arrived = exchanged(pieces, ("x", "tq", "tr"))
    pair = jnp.where(
        c == 0, jnp.concatenate([w_own, w_other], 0), jnp.concatenate([w_other, w_own], 0)
    )
    ring = []
    for k in range(NZ):
        ring += [(k * 2, ((k + 1) % NZ) * 2), (k * 2 + 1, ((k + NZ - 1) % NZ) * 2 + 1)]
    held, wo_own = [pair[:, :768]], pair[:, 768:]
    for _ in range(3):
        held.append(lax.ppermute(held[-1], ("z", "c"), ring))
    same = same_parity()
    swap, one, two, last = [], [], [], []
    for k in range(NZ):
        t = k & 1
        swap.append((k * 2 + 1 - t, k * 2 + t))
        for core, sign in ((0, 1), (1, -1)):
            near, far = (k + sign) % NZ, (k + 2 * sign) % NZ
            one.append(((k * 2 + core) * 2 + t, (near * 2 + core) * 2 + t))
            two.append((k * 2 + core, far * 2 + core))
            if core == 1:
                last.append(((k * 2 + core) * 2 + t, (far * 2 + core) * 2 + t))
    held.append(lax.ppermute(held[2], ("z", "c"), two))
    wo_other = lax.ppermute(wo_own, ("z", "tr"), swap)
    wo_pair = jnp.where(
        lax.axis_index("tr") == 0,
        jnp.concatenate([wo_own, wo_other], 0),
        jnp.concatenate([wo_other, wo_own], 0),
    )
    wo_near = lax.ppermute(wo_pair, ("z", "c", "tr"), one)
    wo_first = jnp.where(same, wo_pair, wo_near)
    wo_second = lax.ppermute(wo_first, ("z", "c"), two)
    wo_third = lax.ppermute(wo_second, ("z", "c", "tr"), last)
    crossed = [moved(held[k], "c") for k in (1, 2, 3)]
    (projected,) = call(
        project,
        [((NX, 768, 128), BF16)],
        arrived,
        *held,
        *crossed,
        scratch=[pltpu.VMEM((1024, 512), BF16)],
        free=range(1, 9),
    )
    (wo_here,) = call(pick, [((512, 512), BF16)], wo_first, wo_second, wo_third)
    shares = exchanged(projected, "x")

    ids = jnp.arange(span_order.shape[0], dtype=jnp.int32)
    own_span = jnp.sum(jnp.where(ids == own, span_order, 0))
    positions = own_span * TOK + jnp.arange(TOK, dtype=jnp.int32)
    half = HEAD // 2
    inverse = jnp.exp(-math.log(ROPE_BASE) * jnp.arange(half, dtype=F32) / half)
    angles = inverse[:, None] * positions.astype(F32)[None, :]
    (residual,) = call(copied, [((128, 512), F32)], hidden_in, far=(0,))
    (bias,) = call(tables, [((768, 128), F32)], bias_query.reshape(1, 512), bias_kv)
    queries, kv = call(
        rotate,
        [((128, 512), BF16), ((NZ, 256, 128), BF16)],
        shares,
        bias,
        jnp.cos(angles),
        jnp.sin(angles),
    )

    wo_there = moved(wo_here, "c")
    kv_here = exchanged(kv, "z")
    others = [moved(queries, "x", step) for step in (1, -1, 2)]
    wo_x = [wo_here] + [moved(wo_here, "x", step) for step in (1, -1, 2)]
    (widened,) = call(copied, [((1, 512), F32)], post_gain.reshape(1, 512))
    kv_there = moved(kv_here, "c")
    (partial,) = call(
        attend,
        [((NX, 144, 512), BF16)],
        span_order,
        queries,
        *others,
        kv_here,
        kv_there,
        scratch=[pltpu.VMEM((2048, 512), F32), pltpu.VMEM((2048, 512), BF16)],
    )
    partial = exchanged(partial, "x")
    wo_c = [wo_there] + [moved(w, "c") for w in wo_x[1:]]
    (gains,) = call(spread, [((8, 512), F32)], widened)
    (attended,) = call(merge, [((512, 128), BF16)], partial)
    attended_other = moved(attended, "tr")
    (out,) = call(
        project_out,
        [((NY // 2, 512, 128), BF16)],
        attended,
        attended_other,
        *wo_x,
        *wo_c,
        scratch=[pltpu.VMEM((2, 512, 128), BF16)],
    )
    out = exchanged(out, "tq")

    attn_out, stream, squares = call(
        mix,
        [((128, 512), BF16), ((128, 512), F32), ((NY, 1, 128), F32)],
        out,
        residual,
        kept=(0,),
    )
    squares = exchanged(squares, TP)
    (normed,) = call(finish, [((128, 512), BF16)], stream, squares, gains, kept=(0,))
    return attn_out, normed


def solution(mesh):
    torus = Mesh(mesh.devices.reshape(NZ, NX, NC, NY // 2, 2), SEQ + TP)
    in_specs = (
        P(SEQ, TP),
        P(),
        P(TP),
        P(SEQ, TP),
        P(TP),
        P(SEQ, None, TP),
        P(None, TP),
        P(TP, SEQ),
        P(TP),
    )
    out_specs = (P(SEQ, TP), P(SEQ, TP))
    return jax.shard_map(
        layer, mesh=torus, in_specs=in_specs, out_specs=out_specs, check_vma=False
    )
```

```python
import functools
import math

import jax
import jax.numpy as jnp
from jax import lax
from jax.experimental import pallas as pl
from jax.experimental.pallas import tpu as pltpu
from jax.sharding import Mesh
from jax.sharding import PartitionSpec as P


MODEL_WIDTH = 4096
HEAD = 128
TOK = 128
GROUP = 4
NZ, NX, NC, NY = 8, 4, 2, 8
SEQ = ("z", "x", "c")
TP = ("tq", "tr")
EPS = 1e-06
ROPE_BASE = 1000000.0
NEG = -(2.0**100)
F32 = jnp.float32
BF16 = jnp.bfloat16


def call(kernel, outs, *args, scratch=(), kept=(), free=(), far=(), limit=24):
    specs, given = [], []
    for k, a in enumerate(args):
        if a.dtype == jnp.int32:
            specs.append(pl.BlockSpec(memory_space=pltpu.SMEM))
        else:
            specs.append(pl.BlockSpec(memory_space=pltpu.VMEM))
            if k not in free:
                space = pltpu.HBM if k in far else pltpu.VMEM
                a = pltpu.with_memory_space_constraint(a, space)
        given.append(a)
    shapes = [
        jax.ShapeDtypeStruct(s, d) if k in kept else pltpu.VMEM(s, d)
        for k, (s, d) in enumerate(outs)
    ]
    spec = [pl.BlockSpec(memory_space=pltpu.VMEM)] * len(outs)
    return pl.pallas_call(
        kernel,
        out_shape=shapes,
        in_specs=specs,
        out_specs=spec,
        scratch_shapes=list(scratch),
        compiler_params=pltpu.CompilerParams(vmem_limit_bytes=limit << 20),
    )(*given)


def split_sum(value):
    high = value.astype(BF16).astype(F32)
    rest = value - high
    middle = rest.astype(BF16).astype(F32)
    return high, middle, (rest - middle)


def rows_of(terms, count):
    width = terms[0].shape[1]
    ids = lax.broadcasted_iota(jnp.int32, (count, width), 0)
    out = jnp.zeros((count, width), F32)
    for k, term in enumerate(terms):
        out = jnp.where(ids == k, jnp.broadcast_to(term, (count, width)), out)
    return out.astype(BF16)


def row_sums(square):
    part = square[:, 0:128] + square[:, 128:256] + square[:, 256:384] + square[:, 384:512]
    return jnp.sum(part.T, axis=0, keepdims=True)


def prepare(h_ref, g_ref, p_ref):
    h = h_ref[...].astype(F32)
    tail = rows_of(split_sum(row_sums(h * h)), 8)
    scaled = (h * g_ref[...].astype(F32).reshape(1, 512)).T
    for x in range(NX):
        block = scaled[x * 128 : (x + 1) * 128, :].astype(BF16)
        for y in range(NY):
            p_ref[x * NY + y, 0:128, :] = block
            p_ref[x * NY + y, 128:136, :] = tail


def stack_weights(wq_ref, wkv_ref, wo_ref, w_ref):
    w_ref[:, 0:512] = wq_ref[...]
    w_ref[:, 512:640] = wkv_ref[:, 0, :]
    w_ref[:, 640:768] = wkv_ref[:, 1, :]
    w_ref[:, 768:1280] = wo_ref[...]


def sources(z, c):
    sign = 2 * c - 1
    near = [z] + [z + sign * k for k in (1, 2, 3, 4)] + [z - sign * k for k in (1, 2, 3)]
    return [(n + NZ) & (NZ - 1) for n in near]


def project(x_ref, *refs):
    w_refs, (out_ref, xs_ref) = refs[:8], refs[8:]
    c = lax.axis_index("c")
    at = sources(lax.axis_index("z"), c)
    scales = []
    for x in range(NX):
        total = jnp.zeros((1, 128), F32)
        for y in range(NY):
            tail = x_ref[x * NY + y, 128:136, :].astype(F32)
            total += tail[0:1] + tail[1:2] + tail[2:3]
        scales.append(lax.rsqrt(total / MODEL_WIDTH + EPS))
    scale = jnp.concatenate(scales, axis=1)
    for k in range(8):
        for x in range(NX):
            block = x_ref[pl.ds(x * NY + at[k], 1), 0:128, :].reshape(128, 128)
            xs_ref[k * 128 : (k + 1) * 128, x * 128 : (x + 1) * 128] = block
    weights = jnp.concatenate([w[...] for w in w_refs], axis=0)
    out = lax.dot_general(
        weights, xs_ref[...], (((0,), (0,)), ((), ())), preferred_element_type=F32
    )
    out = (out * scale).astype(BF16)
    for x in range(NX):
        out_ref[x] = out[:, x * 128 : (x + 1) * 128]


def rotate(r_ref, b_ref, cos_ref, sin_ref, q_ref, kv_ref):
    def total(low, high):
        out = b_ref[low:high, :]
        for x in range(NX):
            out = out + r_ref[x, low:high, :].astype(F32)
        return out

    cos, sin = cos_ref[...], sin_ref[...]

    def turned(head):
        first = total(head * 128, head * 128 + 64)
        second = total(head * 128 + 64, head * 128 + 128)
        return jnp.concatenate(
            [first * cos - second * sin, second * cos + first * sin], axis=0
        )

    for head in range(GROUP):
        q_ref[:, head * 128 : (head + 1) * 128] = turned(head).astype(BF16)
    key = turned(GROUP).T.astype(BF16)
    value = total(640, 768).astype(BF16)
    for z in range(NZ):
        kv_ref[z, 0:128, :] = key
        kv_ref[z, 128:256, :] = value


def attend(order_ref, q0, q1, q2, q3, kv0, kv1, o_ref, s_ref, p_ref):
    z, x, c = (lax.axis_index(a) for a in SEQ)
    key_spans = [order_ref[k * 8 + x * 2 + c] for k in range(NZ)]
    key_spans += [order_ref[k * 8 + x * 2 + 1 - c] for k in range(NZ)]
    values = jnp.concatenate(
        [kv[k, 128:256, :] for kv in (kv0, kv1) for k in range(NZ)], axis=1
    )
    gap = lax.broadcasted_iota(jnp.int32, (128, 512), 0) - (
        lax.broadcasted_iota(jnp.int32, (128, 512), 1) & 127
    )
    factor = math.log2(math.e) / math.sqrt(HEAD)
    for step, q in ((0, q0), (3, q1), (1, q2), (2, q3)):
        owner = (x + step) & 3
        span = order_ref[z * 8 + owner * 2 + c]
        queries = q[...]
        top = jnp.full((8, 512), NEG, F32)
        for k in range(16):
            kv = kv0 if k < 8 else kv1
            s = jnp.dot(kv[k % 8, 0:128, :], queries, preferred_element_type=F32)
            s = jnp.where(gap <= (span - key_spans[k]) * TOK, s * factor, NEG)
            s_ref[k * 128 : (k + 1) * 128, :] = s
            top = jnp.maximum(top, jnp.max(s.reshape(16, 8, 512), axis=0))
        high, low, _ = split_sum(jnp.max(top, axis=0, keepdims=True))
        low = low.astype(BF16).astype(F32)
        peak = high + low
        sums = jnp.zeros((8, 512), F32)
        for k in range(16):
            p = jnp.exp2(s_ref[k * 128 : (k + 1) * 128, :] - peak)
            sums = sums + jnp.sum(p.reshape(16, 8, 512), axis=0)
            p_ref[k * 128 : (k + 1) * 128, :] = p.astype(BF16)
        out = jnp.dot(values, p_ref[...], preferred_element_type=F32)
        total = split_sum(jnp.sum(sums, axis=0, keepdims=True))
        o_ref[pl.ds(owner, 1), 0:128, :] = out.astype(BF16)[None]
        o_ref[pl.ds(owner, 1), 128:144, :] = rows_of((high, low) + total, 16)[None]


def same_parity():
    return (lax.axis_index("z") & 1) == lax.axis_index("tr")


def pick(h1, h2, h3, out_ref):
    late = jnp.logical_and(same_parity(), lax.axis_index("c") == 1)

    @pl.when(late)
    def _():
        out_ref[0:256, :] = h2[...]
        out_ref[256:512, :] = h3[...]

    @pl.when(jnp.logical_not(late))
    def _():
        out_ref[0:256, :] = h1[...]
        out_ref[256:512, :] = h2[...]


def tables(bq_ref, bkv_ref, b_ref):
    for k in range(4):
        row = bq_ref[:, k * 128 : (k + 1) * 128].astype(F32)
        b_ref[k * 128 : (k + 1) * 128, :] = jnp.broadcast_to(row, (128, 128)).T
    for k in range(2):
        row = bkv_ref[k : k + 1, :].astype(F32)
        b_ref[512 + k * 128 : 640 + k * 128, :] = jnp.broadcast_to(row, (128, 128)).T


def merge(o_ref, a_ref):
    tails = [o_ref[k, 128:144, :].astype(F32) for k in range(NX)]
    peaks = [t[0:1] + t[1:2] for t in tails]
    top = functools.reduce(jnp.maximum, peaks)
    shares = [jnp.exp2(peak - top) for peak in peaks]
    total = sum(s * (t[2:3] + t[3:4] + t[4:5]) for s, t in zip(shares, tails))
    out = sum(s * o_ref[k, 0:128, :].astype(F32) for k, s in enumerate(shares)) / total
    out = out.astype(BF16)
    for head in range(GROUP):
        a_ref[head * 128 : (head + 1) * 128, :] = out[:, head * 128 : (head + 1) * 128]


def half_rows(w_refs, side):
    rows = []
    for w in w_refs:
        for n in range(2):
            rows.append(w[pl.ds(pl.multiple_of(n * 256 + side * 128, 128), 128), :])
    return jnp.concatenate(rows, axis=0)


def project_half(a_own, *refs):
    w_refs, sum_ref = refs[:8], refs[8]
    sum_ref[...] = jnp.dot(
        half_rows(w_refs, lax.axis_index("tr")), a_own[...], preferred_element_type=F32
    )


def project_out(sum_ref, a_other, *refs):
    w_refs, out_ref = refs[:8], refs[8]
    z, x, c = (lax.axis_index(a) for a in SEQ)
    same = jnp.where(same_parity(), 1, 0)
    low, high = z - 1 + same, z + 1 + same
    part = jnp.dot(
        half_rows(w_refs, 1 - lax.axis_index("tr")), a_other[...], preferred_element_type=F32
    )
    part = (sum_ref[...] + part).astype(BF16)
    for core in range(2):
        for k in range(4):
            owner = (x + (0, 3, 1, 2)[k]) & 3
            cols = pl.ds(pl.multiple_of(owner * 128, 128), 128)
            for n in range(2):
                block = jnp.where(c == core, low - 2 * n, high + 2 * n)
                y = ((block + NZ) & (NZ - 1)) >> 1
                at = (core * 8 + k * 2 + n) * 128
                out_ref[pl.ds(y, 1), cols, :] = part[at : at + 128, :][None]


def copied(in_ref, out_ref):
    out_ref[...] = in_ref[...].astype(F32)


def spread(in_ref, out_ref):
    out_ref[...] = jnp.broadcast_to(in_ref[...], (8, 512))


def mix(part_ref, h_ref, attn_ref, stream_ref, sq_ref):
    mixed = part_ref[0].astype(F32)
    for y in range(1, NY // 2):
        mixed = mixed + part_ref[y].astype(F32)
    mixed = mixed.T
    attn_ref[...] = mixed.astype(BF16)
    stream = h_ref[...] + mixed
    stream_ref[...] = stream
    sums = row_sums(stream * stream)
    for y in range(NY):
        sq_ref[y] = sums


def finish(stream_ref, sq_ref, g_ref, out_ref):
    total = sq_ref[0]
    for y in range(1, NY):
        total = total + sq_ref[y]
    scale = lax.rsqrt(total / MODEL_WIDTH + EPS)
    scale = jnp.broadcast_to(scale, (128, 128)).T
    gain = g_ref[0:1, :]
    for k in range(4):
        cols = slice(k * 128, (k + 1) * 128)
        out_ref[:, cols] = (stream_ref[:, cols] * scale * gain[:, cols]).astype(BF16)


def shifted(array, axis, step):
    size = lax.axis_size(axis)
    return lax.ppermute(array, axis, [(i, (i + step) % size) for i in range(size)])


def exchanged(array, axis):
    return lax.all_to_all(array, axis, 0, 0, tiled=True)


def moved(array, axis, step=1):
    return shifted(array, axis, step)


def layer(
    hidden_in,
    span_order,
    norm_gain,
    w_query,
    bias_query,
    key_value_weight,
    bias_kv,
    w_out,
    post_gain,
):
    z, x, c = (lax.axis_index(a) for a in SEQ)
    own = z * 8 + x * 2 + c

    (w_own,) = call(
        stack_weights,
        [((64, 1280), BF16)],
        w_query,
        key_value_weight,
        w_out.T,
        far=(0, 1, 2),
    )
    w_other = moved(w_own, "c")
    (pieces,) = call(
        prepare, [((NX * NY, 136, 128), BF16)], hidden_in, norm_gain, far=(0, 1)
    )
    arrived = exchanged(pieces, ("x", "tq", "tr"))
    pair = jnp.where(
        c == 0, jnp.concatenate([w_own, w_other], 0), jnp.concatenate([w_other, w_own], 0)
    )
    ring = []
    for k in range(NZ):
        ring += [(k * 2, ((k + 1) % NZ) * 2), (k * 2 + 1, ((k + NZ - 1) % NZ) * 2 + 1)]
    held, wo_own = [pair[:, :768]], pair[:, 768:]
    for _ in range(3):
        held.append(lax.ppermute(held[-1], ("z", "c"), ring))
    same = same_parity()
    swap, one, two, last = [], [], [], []
    for k in range(NZ):
        t = k & 1
        swap.append((k * 2 + 1 - t, k * 2 + t))
        for core, sign in ((0, 1), (1, -1)):
            near, far = (k + sign) % NZ, (k + 2 * sign) % NZ
            one.append(((k * 2 + core) * 2 + t, (near * 2 + core) * 2 + t))
            two.append((k * 2 + core, far * 2 + core))
            if core == 1:
                last.append(((k * 2 + core) * 2 + t, (far * 2 + core) * 2 + t))
    held.append(lax.ppermute(held[2], ("z", "c"), two))
    wo_other = lax.ppermute(wo_own, ("z", "tr"), swap)
    wo_pair = jnp.where(
        lax.axis_index("tr") == 0,
        jnp.concatenate([wo_own, wo_other], 0),
        jnp.concatenate([wo_other, wo_own], 0),
    )
    wo_near = lax.ppermute(wo_pair, ("z", "c", "tr"), one)
    wo_first = jnp.where(same, wo_pair, wo_near)
    wo_second = lax.ppermute(wo_first, ("z", "c"), two)
    wo_third = lax.ppermute(wo_second, ("z", "c", "tr"), last)
    crossed = [moved(held[k], "c") for k in (1, 2, 3)]
    (projected,) = call(
        project,
        [((NX, 768, 128), BF16)],
        arrived,
        *held,
        *crossed,
        scratch=[pltpu.VMEM((1024, 512), BF16)],
        free=range(1, 9),
    )
    (wo_here,) = call(pick, [((512, 512), BF16)], wo_first, wo_second, wo_third)
    shares = exchanged(projected, "x")

    ids = jnp.arange(span_order.shape[0], dtype=jnp.int32)
    own_span = jnp.sum(jnp.where(ids == own, span_order, 0))
    positions = own_span * TOK + jnp.arange(TOK, dtype=jnp.int32)
    half = HEAD // 2
    inverse = jnp.exp(-math.log(ROPE_BASE) * jnp.arange(half, dtype=F32) / half)
    angles = inverse[:, None] * positions.astype(F32)[None, :]
    (residual,) = call(copied, [((128, 512), F32)], hidden_in, far=(0,))
    (bias,) = call(tables, [((768, 128), F32)], bias_query.reshape(1, 512), bias_kv)
    queries, kv = call(
        rotate,
        [((128, 512), BF16), ((NZ, 256, 128), BF16)],
        shares,
        bias,
        jnp.cos(angles),
        jnp.sin(angles),
    )

    wo_there = moved(wo_here, "c")
    kv_here = exchanged(kv, "z")
    others = [moved(queries, "x", step) for step in (1, -1, 2)]
    wo_x = [wo_here] + [moved(wo_here, "x", step) for step in (1, -1, 2)]
    (widened,) = call(copied, [((1, 512), F32)], post_gain.reshape(1, 512))
    kv_there = moved(kv_here, "c")
    (partial,) = call(
        attend,
        [((NX, 144, 512), BF16)],
        span_order,
        queries,
        *others,
        kv_here,
        kv_there,
        scratch=[pltpu.VMEM((2048, 512), F32), pltpu.VMEM((2048, 512), BF16)],
    )
    partial = exchanged(partial, "x")
    wo_c = [wo_there] + [moved(w, "c") for w in wo_x[1:]]
    (gains,) = call(spread, [((8, 512), F32)], widened)
    (attended,) = call(merge, [((512, 128), BF16)], partial)
    attended_other = moved(attended, "tr")
    (half,) = call(
        project_half, [((2048, 128), F32)], attended, *wo_x, *wo_c, free=range(1, 9)
    )
    (out,) = call(
        project_out,
        [((NY // 2, 512, 128), BF16)],
        half,
        attended_other,
        *wo_x,
        *wo_c,
        free=range(2, 10),
    )
    out = exchanged(out, "tq")

    attn_out, stream, squares = call(
        mix,
        [((128, 512), BF16), ((128, 512), F32), ((NY, 1, 128), F32)],
        out,
        residual,
        kept=(0,),
    )
    squares = exchanged(squares, TP)
    (normed,) = call(finish, [((128, 512), BF16)], stream, squares, gains, kept=(0,))
    return attn_out, normed


def solution(mesh):
    torus = Mesh(mesh.devices.reshape(NZ, NX, NC, NY // 2, 2), SEQ + TP)
    in_specs = (
        P(SEQ, TP),
        P(),
        P(TP),
        P(SEQ, TP),
        P(TP),
        P(SEQ, None, TP),
        P(None, TP),
        P(TP, SEQ),
        P(TP),
    )
    out_specs = (P(SEQ, TP), P(SEQ, TP))
    return jax.shard_map(
        layer, mesh=torus, in_specs=in_specs, out_specs=out_specs, check_vma=False
    )
```
